32 devices in a mesh: row: 4 (over z), col: 8 (over y, x, core).
Axes of the slice: x: 2, y: 2, z: 4, core: 2. Of those that a mesh axis runs over, the one named last changes fastest.
Arguments:
- right_side: float32 [256, 2048], P('row', 'col'), may hold values from -20 to 20
- initial_guess: float32 [256, 2048], P('row', 'col'), may hold values from -3 to 3
- kernel: float32 [31, 31], replicated, may hold values from 0 to 1, as said below
Outputs:
- template: float32 [256, 2048], P('row', 'col')
- residual: float32 [256, 2048], P('row', 'col')
The draws below stay inside these ranges and needn't reach their ends.
Inputs may be any that keep to these rules, and one draw needn't show every extreme that they name: `kernel`: entries are positive and sum to one.
All inputs are finite; a program needn't handle non-finite values.
Results may differ from the reference program's by a relative error of at most 0.0003.
Values sent between devices are 32-bit elements; how exact they have to be, the bound alone decides.
No kernel may reach another device: no remote copies, remote signals or barrier semaphores. Data moves between devices by JAX's collectives and lax.ppermute only.
A program may use at most 128 MiB of HBM per device.

```python
import jax
import jax.numpy as jnp

KW = 31
ITERS = 3
NX = 256
NY = 2048


def draw_right_side(key, part):
    rough = jax.random.normal(jax.random.fold_in(key, 11), (NX, NY), jnp.float32)
    column_pos = jnp.arange(NY, dtype=jnp.float32) / max(NY - 1, 1)
    ramp = jnp.exp(jnp.log(3.0) * column_pos)[None, :]
    values = rough * ramp
    return jnp.clip(values, -20.0, 20.0)


def draw_kernel(key, part):
    center = (KW - 1) / 2.0
    offsets = jnp.arange(KW, dtype=jnp.float32) - center
    radius_sq = offsets[:, None] ** 2 + offsets[None, :] ** 2
    profile = jnp.exp(-radius_sq / 98.0)
    factor = jax.random.uniform(jax.random.fold_in(key, 21), (KW, KW), jnp.float32, 0.5, 1.5)
    weights = profile * factor
    return weights / jnp.sum(weights)


def shard_levels(own_key, shape, shards, least, largest):
    def one(position, blocks):
        draws = jax.random.uniform(jax.random.fold_in(jax.random.fold_in(own_key, 6), position), (blocks,), jnp.float32, least / len(shards), largest / len(shards))
        return jnp.repeat(jnp.exp(draws), shape[position] // blocks).reshape((-1,) + (1,) * (len(shape) - position - 1))

    gain = one(*shards[0])
    for cut in shards[1:]:
        gain = gain * one(*cut)
    return gain


def scatter_about(rng, dims, deviation, bound, split=(), kind=jnp.bfloat16):
    level = shard_levels(rng, dims, split, -0.22, 0.18) if split else 1.0
    result = jax.random.normal(rng, dims, jnp.float32) * deviation * level
    return jnp.minimum(jnp.maximum(result, -bound), bound).astype(kind)


def setup_inputs(seed: int = 0) -> dict:
    splits = jax.random.split(jax.random.key(seed), 4)
    return {
        "right_side": draw_right_side(jax.random.fold_in(splits[3], 71), 0),
        "initial_guess": scatter_about(splits[1], (NX, NY), 0.5, 3.0, ((0, 4), (1, 8)), jnp.float32),
        "kernel": draw_kernel(jax.random.fold_in(splits[3], 71), 0),
    }


penalty = 0.05


def convolve(source, taps):
    half_width = taps.shape[0] // 2
    tile_rows, tile_cols = source.shape
    extent = (tile_rows + 2 * half_width, tile_cols + 2 * half_width)
    spectrum = jnp.fft.rfft2(source, s=extent) * jnp.fft.rfft2(taps, s=extent)
    complete = jnp.fft.irfft2(spectrum, s=extent)
    return complete[half_width:half_width + tile_rows, half_width:half_width + tile_cols].astype(source.dtype)


def laplacian(source):
    padded = jnp.pad(source, 1)
    return 4.0 * source - padded[2:, 1:-1] - padded[:-2, 1:-1] - padded[1:-1, 2:] - padded[1:-1, :-2]


def operate(source, kernel):
    blurred = convolve(source, kernel[::-1, ::-1])
    return convolve(blurred, kernel) + penalty * laplacian(source)


def reference(right_side, initial_guess, kernel):
    template = initial_guess
    residual = right_side - operate(template, kernel)
    direction = residual
    norm_now = jnp.sum(residual * residual)
    for iteration in range(ITERS):
        applied = operate(direction, kernel)
        step_size = norm_now / jnp.sum(direction * applied)
        template = template + step_size * direction
        residual = residual - step_size * applied
        norm_next = jnp.sum(residual * residual)
        direction = residual + (norm_next / norm_now) * direction
        norm_now = norm_next
    return template, residual
```

```python
import jax
import jax.numpy as jnp
from jax import lax
from jax.experimental import pallas as pl
from jax.experimental.pallas import tpu as pltpu
from jax.sharding import PartitionSpec as P

ITERS = 3
PENALTY = 0.05
LANES = 128
SHIFTS = 4
BLOCK = 32
BAND = 64
EDGE = 16
BASIS = ITERS + 1
PAIRS = [(i, j) for i in range(BASIS) for j in range(i, BASIS)]


def round_up(value, step):
    return -(-value // step) * step


def two_sum(a, b):
    s = a + b
    t = s - a
    return s, (a - (s - t)) + (b - t)


def halves(a):
    c = a * 4097.0
    high = c - (c - a)
    return high, a - high


def two_prod(a, b):
    p = a * b
    ah, al = halves(a)
    bh, bl = halves(b)
    return p, ((ah * bh - p) + ah * bl + al * bh) + al * bl


def dd_add(x, y):
    s, e = two_sum(x[0], y[0])
    return two_sum(s, e + (x[1] + y[1]))


def dd_mul(x, y):
    p, e = two_prod(x[0], y[0])
    return two_sum(p, e + (x[0] * y[1] + x[1] * y[0]))


def dd_neg(x):
    return -x[0], -x[1]


def dd_div(x, y):
    q = x[0] / y[0]
    rest = dd_add(x, dd_neg(dd_mul((q, jnp.zeros_like(q)), y)))
    return two_sum(q, rest[0] / y[0])


def toeplitz_tables(taps):
    width = taps.shape[0]
    groups = -(-width // SHIFTS)
    skip = EDGE - width // 2
    tap = jnp.arange(width, dtype=jnp.int32)[:, None, None]
    row = jnp.arange(BLOCK, dtype=jnp.int32)[None, :, None]
    band = jnp.arange(BAND, dtype=jnp.int32)[None, None, :]
    selector = (band - row - skip == tap).astype(jnp.float32)
    both = jnp.stack([taps, taps[::-1, ::-1]])
    both = jnp.pad(both, ((0, 0), (0, 0), (0, groups * SHIFTS - width)))
    both = both.reshape(2, width, groups, SHIFTS)
    tables = jnp.einsum("zags,arq->zgrsq", both, selector, precision=lax.Precision.HIGHEST)
    return tables.reshape(2, groups * BLOCK, SHIFTS * BAND)


def krylov(xb, tables, start, *, half, own, columns, x_lanes, interpret=False):
    rows = xb.shape[0]
    groups = tables.shape[1] // BLOCK
    halo = 2 * half * BASIS
    x_width = own + 2 * halo
    tall = rows + 2 * EDGE

    def body(start_ref, xb_ref, t_ref, v_ref, g_ref, pad, stack, out, smooth, taps):
        for which in range(2):
            full = t_ref[which]
            high = full.astype(jnp.bfloat16)
            low = (full - high.astype(jnp.float32)).astype(jnp.bfloat16)
            span = full.shape[1]
            taps[which, :, 0:span] = high
            taps[which, :, span : 2 * span] = low
            taps[which, :, 2 * span : 3 * span] = high
        pad[0:EDGE, :] = jnp.zeros((EDGE, x_lanes), jnp.float32)
        pad[EDGE + rows : tall, :] = jnp.zeros((EDGE, x_lanes), jnp.float32)

        def correlate(which, lanes):
            for shift in range(SHIFTS):
                moved = pad[:, 0:lanes]
                if shift:
                    moved = pltpu.roll(moved, lanes - shift, 1)
                high = moved.astype(jnp.bfloat16)
                stack[0, shift, :, 0:lanes] = high
                stack[1, shift, :, 0:lanes] = (moved - high.astype(jnp.float32)).astype(
                    jnp.bfloat16
                )

            def one(block):
                base = pl.multiple_of(block * BLOCK, BLOCK)
                operand = jnp.concatenate(
                    [
                        stack[part, shift, pl.ds(base, BAND), 0:lanes]
                        for part in (0, 0, 1)
                        for shift in range(SHIFTS)
                    ],
                    axis=0,
                )
                acc = jnp.dot(taps[which], operand, preferred_element_type=jnp.float32)
                total = acc[(groups - 1) * BLOCK :]
                for group in range(groups - 2, -1, -1):
                    total = acc[group * BLOCK : (group + 1) * BLOCK] + pltpu.roll(
                        total, lanes - SHIFTS, 1
                    )
                out[pl.ds(base, BLOCK), 0:lanes] = total

            def step(pair, carry):
                one(2 * pair)
                one(2 * pair + 1)
                return carry

            lax.fori_loop(0, rows // (2 * BLOCK), step, 0)

        def inside(value, first, width):
            lane = lax.broadcasted_iota(jnp.int32, value.shape, 1)
            position = lane + first
            keep = (position >= 0) & (position < columns) & (lane < width)
            return jnp.where(keep, value, 0.0)

        def operate(source, first, width):
            lanes = round_up(width, LANES)
            pad[EDGE : EDGE + rows, 0:lanes] = source
            center = pad[EDGE : EDGE + rows, 0:lanes]
            lap = (
                4.0 * center
                - pad[EDGE - 1 : EDGE - 1 + rows, 0:lanes]
                - pad[EDGE + 1 : EDGE + 1 + rows, 0:lanes]
                - pltpu.roll(center, 1, 1)
                - pltpu.roll(center, lanes - 1, 1)
            )
            smooth[:, 0:lanes] = PENALTY * pltpu.roll(lap, lanes - 2 * half, 1)
            correlate(0, lanes)
            inner = width - 2 * half
            lanes_in = round_up(inner, LANES)
            pad[EDGE : EDGE + rows, 0:lanes_in] = inside(
                out[:, 0:lanes_in], first + half, inner
            )
            correlate(1, lanes_in)
            last = width - 4 * half
            lanes_out = round_up(last, LANES)
            return out[:, 0:lanes_out] + smooth[:, 0:lanes_out], last

        first = start_ref[0]
        width = x_width
        x = xb_ref[:, 0:x_lanes]
        applied, last = operate(x, first, width)
        vector = xb_ref[:, x_lanes : x_lanes + applied.shape[1]] - applied
        kept = []
        lane = lax.broadcasted_iota(jnp.int32, (rows, LANES), 1)

        def own_part(value, margin):
            lanes = value.shape[1]
            if margin:
                value = pltpu.roll(value, lanes - margin, 1)
            return jnp.where(lane < own, value[:, 0:LANES], 0.0)

        v_ref[BASIS] = own_part(x, halo)
        for index in range(BASIS):
            first = first + 2 * half
            width = last
            vector = inside(vector, first, width)
            part = own_part(vector, (width - own) // 2)
            v_ref[index] = part
            if index + 1 < BASIS:
                vector, last = operate(vector, first, width)

        lane8 = lax.broadcasted_iota(jnp.int32, (8, LANES), 1)
        sub8 = lax.broadcasted_iota(jnp.int32, (8, LANES), 0)
        gram = jnp.zeros((8, LANES), jnp.float32)
        for slot, (i, j) in enumerate(PAIRS):
            value = two_prod(v_ref[i], v_ref[j])
            count = rows
            while count > 8:
                count //= 2
                value = dd_add(
                    (value[0][:count], value[1][:count]), (value[0][count:], value[1][count:])
                )
            for axis, size in ((0, 8), (1, LANES)):
                step = size // 2
                while step:
                    value = dd_add(
                        value, tuple(pltpu.roll(part, step, axis) for part in value)
                    )
                    step //= 2
            gram = jnp.where((lane8 == slot) & (sub8 == 0), value[0], gram)
            gram = jnp.where((lane8 == slot) & (sub8 == 1), value[1], gram)
        g_ref[...] = gram

    vmem = pl.BlockSpec(memory_space=pltpu.VMEM)
    return pl.pallas_call(
        body,
        in_specs=[pl.BlockSpec(memory_space=pltpu.SMEM), vmem, vmem],
        out_specs=[vmem, vmem],
        out_shape=[
            jax.ShapeDtypeStruct((BASIS + 1, rows, LANES), jnp.float32),
            jax.ShapeDtypeStruct((8, LANES), jnp.float32),
        ],
        scratch_shapes=[
            pltpu.VMEM((tall, x_lanes), jnp.float32),
            pltpu.VMEM((2, SHIFTS, tall, x_lanes), jnp.bfloat16),
            pltpu.VMEM((rows, x_lanes), jnp.float32),
            pltpu.VMEM((rows, x_lanes), jnp.float32),
            pltpu.VMEM((2, groups * BLOCK, 3 * SHIFTS * BAND), jnp.bfloat16),
        ],
        name="krylov",
        interpret=interpret,
    )(start, xb, tables)


def combine(vectors, grams, *, own, interpret=False):
    rows = vectors.shape[1]
    members = grams.shape[0]

    def body(v_ref, g_ref, o_ref):
        high = jnp.concatenate([g_ref[m, 0:1] for m in range(members)], axis=0)
        low = jnp.concatenate([g_ref[m, 1:2] for m in range(members)], axis=0)
        total = (high, low)
        count = members
        while count > 1:
            count //= 2
            total = dd_add(
                (total[0][:count], total[1][:count]), (total[0][count:], total[1][count:])
            )
        entries = {}
        for slot, (i, j) in enumerate(PAIRS):
            entry = tuple(
                jnp.broadcast_to(part[:, slot : slot + 1], (1, LANES)) for part in total
            )
            entries[i, j] = entries[j, i] = entry

        def inner(p, q, ahead):
            result = None
            for i, a in enumerate(p):
                row = None
                for j, b in enumerate(q):
                    term = dd_mul(b, entries[i, j + ahead])
                    row = term if row is None else dd_add(row, term)
                row = dd_mul(a, row)
                result = row if result is None else dd_add(result, row)
            return result

        one = (jnp.ones((1, LANES), jnp.float32), jnp.zeros((1, LANES), jnp.float32))
        residual = [one]
        direction = [one]
        template = []
        norm_now = entries[0, 0]
        for iteration in range(ITERS):
            step_size = dd_div(norm_now, inner(direction, direction, 1))
            moved = [dd_mul(step_size, d) for d in direction]
            template = [dd_add(t, m) for t, m in zip(template, moved)] + moved[len(template) :]
            residual = (
                residual[:1]
                + [dd_add(r, dd_neg(m)) for r, m in zip(residual[1:], moved)]
                + [dd_neg(m) for m in moved[len(residual) - 1 :]]
            )
            if iteration + 1 < ITERS:
                norm_next = inner(residual, residual, 0)
                ratio = dd_div(norm_next, norm_now)
                scaled = [dd_mul(ratio, d) for d in direction]
                direction = [dd_add(r, s) for r, s in zip(residual, scaled)] + residual[
                    len(scaled) :
                ]
                norm_now = norm_next
        final = v_ref[BASIS]
        for index, weight in enumerate(template):
            final = final + weight[0] * v_ref[index]
        rest = v_ref[0] * residual[0][0]
        for index in range(1, BASIS):
            rest = rest + residual[index][0] * v_ref[index]
        lane = lax.broadcasted_iota(jnp.int32, (rows, LANES), 1)
        o_ref[...] = jnp.where(lane < own, final, pltpu.roll(rest, own, 1))

    vmem = pl.BlockSpec(memory_space=pltpu.VMEM)
    return pl.pallas_call(
        body,
        in_specs=[vmem, vmem],
        out_specs=vmem,
        out_shape=jax.ShapeDtypeStruct((rows, LANES), jnp.float32),
        name="combine",
        interpret=interpret,
    )(vectors, grams)


def on_device(right_side, initial_guess, kernel):
    tile_rows, tile_cols = initial_guess.shape
    row_count = lax.axis_size("row")
    col_count = lax.axis_size("col")
    half = kernel.shape[0] // 2
    own = tile_cols // row_count
    halo = 2 * half * BASIS
    side = halo - 2 * half
    x_lanes = round_up(own + 2 * halo, LANES)
    b_lanes = round_up(own + 2 * side, LANES)

    up = [(i, i + 1) for i in range(col_count - 1)]
    down = [(j, i) for i, j in up]
    right_edge = jnp.concatenate([initial_guess[:, -halo:], right_side[:, -side:]], axis=1)
    left_edge = jnp.concatenate([initial_guess[:, :halo], right_side[:, :side]], axis=1)
    before = lax.ppermute(right_edge, "col", up)
    after = lax.ppermute(left_edge, "col", down)
    tables = toeplitz_tables(kernel)
    x = jnp.concatenate([before[:, :halo], initial_guess, after[:, :halo]], axis=1)
    b = jnp.concatenate([before[:, halo:], right_side, after[:, halo:]], axis=1)
    x = jnp.pad(x, ((0, 0), (0, (row_count - 1) * own + x_lanes - x.shape[1])))
    b = jnp.pad(b, ((0, 0), (0, max(0, (row_count - 1) * own + b_lanes - b.shape[1]))))
    blocks = jnp.stack(
        [
            jnp.concatenate(
                [x[:, i * own : i * own + x_lanes], b[:, i * own : i * own + b_lanes]], axis=1
            )
            for i in range(row_count)
        ]
    )
    slab = lax.all_to_all(blocks, "row", 0, 0).reshape(row_count * tile_rows, x_lanes + b_lanes)
    start = lax.axis_index("col") * tile_cols + lax.axis_index("row") * own - halo
    vectors, gram = krylov(
        slab,
        tables,
        start.astype(jnp.int32).reshape(1),
        half=half,
        own=own,
        columns=col_count * tile_cols,
        x_lanes=x_lanes,
    )
    members = row_count * col_count
    sent = jnp.broadcast_to(gram[None], (members,) + gram.shape)
    grams = lax.all_to_all(sent, ("row", "col"), 0, 0)
    both = combine(vectors, grams, own=own)
    back = both[:, : 2 * own].reshape(row_count, tile_rows, 2 * own)
    back = lax.all_to_all(back, "row", 0, 0)
    template = jnp.concatenate([back[i, :, :own] for i in range(row_count)], axis=1)
    residual = jnp.concatenate([back[i, :, own:] for i in range(row_count)], axis=1)
    return (template, residual)


def solution(mesh):
    placed = (P("row", "col"), P("row", "col"), P())
    return jax.shard_map(
        on_device,
        mesh=mesh,
        in_specs=placed,
        out_specs=(P("row", "col"), P("row", "col")),
        check_vma=False,
    )
```

```python
import math

import jax
import jax.numpy as jnp
from jax import lax
from jax.experimental import pallas as pl
from jax.experimental.pallas import tpu as pltpu
from jax.sharding import PartitionSpec as P

ITERS = 3
PENALTY = 0.05
LANES = 128
SHIFTS = 4
BLOCK = 32
BAND = 64
UNROLL = 2
EDGE = 16
BASIS = ITERS + 1
PAIRS = [(i, j) for i in range(BASIS) for j in range(i, BASIS)]


def round_up(value, step):
    return -(-value // step) * step


def two_sum(a, b):
    s = a + b
    t = s - a
    return s, (a - (s - t)) + (b - t)


def halves(a):
    c = a * 4097.0
    high = c - (c - a)
    return high, a - high


def two_prod(a, b):
    p = a * b
    ah, al = halves(a)
    bh, bl = halves(b)
    return p, ((ah * bh - p) + ah * bl + al * bh) + al * bl


def dd_add(x, y):
    s, e = two_sum(x[0], y[0])
    return two_sum(s, e + (x[1] + y[1]))


def dd_mul(x, y):
    p, e = two_prod(x[0], y[0])
    return two_sum(p, e + (x[0] * y[1] + x[1] * y[0]))


def dd_neg(x):
    return -x[0], -x[1]


def dd_div(x, y):
    q = x[0] / y[0]
    rest = dd_add(x, dd_neg(dd_mul((q, jnp.zeros_like(q)), y)))
    return two_sum(q, rest[0] / y[0])


def toeplitz_tables(taps):
    width = taps.shape[0]
    groups = -(-width // SHIFTS)
    skip = EDGE - width // 2
    tap = jnp.arange(width, dtype=jnp.int32)[:, None, None]
    row = jnp.arange(BLOCK, dtype=jnp.int32)[None, :, None]
    band = jnp.arange(BAND, dtype=jnp.int32)[None, None, :]
    selector = (band - row - skip == tap).astype(jnp.float32)
    both = jnp.stack([taps, taps[::-1, ::-1]])
    both = jnp.pad(both, ((0, 0), (0, 0), (0, groups * SHIFTS - width)))
    both = both.reshape(2, width, groups, SHIFTS)
    tables = jnp.einsum("zags,arq->zgrsq", both, selector, precision=lax.Precision.HIGHEST)
    return tables.reshape(2, groups * BLOCK, SHIFTS * BAND)


class Slab:
    def __init__(self, rows, half, columns, pad, stack, out, smooth, taps):
        self.rows, self.half, self.columns = rows, half, columns
        self.pad, self.stack, self.out, self.smooth, self.taps = pad, stack, out, smooth, taps
        lanes = pad.shape[1]
        pad[0:EDGE, :] = jnp.zeros((EDGE, lanes), jnp.float32)
        pad[EDGE + rows :, :] = jnp.zeros((EDGE, lanes), jnp.float32)

    @staticmethod
    def scratch(rows, lanes):
        tall = rows + 2 * EDGE
        return [
            pltpu.VMEM((tall, lanes), jnp.float32),
            pltpu.VMEM((2, SHIFTS, tall, lanes), jnp.bfloat16),
            pltpu.VMEM((rows, lanes), jnp.float32),
            pltpu.VMEM((rows, lanes), jnp.float32),
        ]

    def correlate(self, which, lanes):
        pad, stack, out, taps = self.pad, self.stack, self.out, self.taps
        groups = taps.shape[1] // BLOCK
        for shift in range(SHIFTS):
            moved = pad[:, 0:lanes]
            if shift:
                moved = pltpu.roll(moved, lanes - shift, 1)
            high = moved.astype(jnp.bfloat16)
            stack[0, shift, :, 0:lanes] = high
            stack[1, shift, :, 0:lanes] = (moved - high.astype(jnp.float32)).astype(jnp.bfloat16)

        def one(block):
            base = pl.multiple_of(block * BLOCK, BLOCK)
            operand = jnp.concatenate(
                [
                    stack[part, shift, pl.ds(base, BAND), 0:lanes]
                    for part in (0, 0, 1)
                    for shift in range(SHIFTS)
                ],
                axis=0,
            )
            acc = jnp.dot(taps[which], operand, preferred_element_type=jnp.float32)
            total = acc[(groups - 1) * BLOCK :]
            for group in range(groups - 2, -1, -1):
                total = acc[group * BLOCK : (group + 1) * BLOCK] + pltpu.roll(
                    total, lanes - SHIFTS, 1
                )
            out[pl.ds(base, BLOCK), 0:lanes] = total

        count = self.rows // BLOCK
        together = math.gcd(count, UNROLL)

        def step(turn, carry):
            for index in range(together):
                one(together * turn + index)
            return carry

        lax.fori_loop(0, count // together, step, 0)

    def inside(self, value, first, width):
        lane = lax.broadcasted_iota(jnp.int32, value.shape, 1)
        position = lane + first
        keep = (position >= 0) & (position < self.columns) & (lane < width)
        return jnp.where(keep, value, 0.0)

    def operate(self, source, first, width):
        rows, half, pad = self.rows, self.half, self.pad
        lanes = round_up(width, LANES)
        pad[EDGE : EDGE + rows, 0:lanes] = source
        center = pad[EDGE : EDGE + rows, 0:lanes]
        lap = (
            4.0 * center
            - pad[EDGE - 1 : EDGE - 1 + rows, 0:lanes]
            - pad[EDGE + 1 : EDGE + 1 + rows, 0:lanes]
            - pltpu.roll(center, 1, 1)
            - pltpu.roll(center, lanes - 1, 1)
        )
        self.smooth[:, 0:lanes] = PENALTY * pltpu.roll(lap, lanes - 2 * half, 1)
        self.correlate(0, lanes)
        inner = width - 2 * half
        lanes_in = round_up(inner, LANES)
        pad[EDGE : EDGE + rows, 0:lanes_in] = self.inside(
            self.out[:, 0:lanes_in], first + half, inner
        )
        self.correlate(1, lanes_in)
        last = width - 4 * half
        lanes_out = round_up(last, LANES)
        return self.out[:, 0:lanes_out] + self.smooth[:, 0:lanes_out]


def specs(*spaces):
    return [pl.BlockSpec(memory_space=space) for space in spaces]


def apply_first(x, tables, start, *, half, columns, width):
    rows, lanes = x.shape
    span = tables.shape[2]
    last = round_up(width - 4 * half, LANES)

    def body(start_ref, x_ref, t_ref, o_ref, taps, *scratch):
        for which in range(2):
            full = t_ref[which]
            high = full.astype(jnp.bfloat16)
            low = (full - high.astype(jnp.float32)).astype(jnp.bfloat16)
            taps[which, :, 0:span] = high
            taps[which, :, span : 2 * span] = low
            taps[which, :, 2 * span : 3 * span] = high
        slab = Slab(rows, half, columns, *scratch, taps)
        o_ref[...] = slab.operate(x_ref[...], start_ref[0], width)

    return pl.pallas_call(
        body,
        in_specs=specs(pltpu.SMEM, pltpu.VMEM, pltpu.VMEM),
        out_specs=specs(pltpu.VMEM, pltpu.VMEM),
        out_shape=[
            jax.ShapeDtypeStruct((rows, last), jnp.float32),
            jax.ShapeDtypeStruct((2, tables.shape[1], 3 * span), jnp.bfloat16),
        ],
        scratch_shapes=Slab.scratch(rows, lanes),
        name="apply_first",
    )(start, x, tables)


def krylov(b, applied, taps, start, *, half, own, columns, width):
    rows, lanes = b.shape
    per_row = BASIS * own

    def body(start_ref, b_ref, a_ref, t_ref, v_ref, g_ref, basis, *scratch):
        slab = Slab(rows, half, columns, *scratch, t_ref)
        first = start_ref[0]
        wide = width
        vector = b_ref[...] - a_ref[...]
        lane = lax.broadcasted_iota(jnp.int32, (rows, LANES), 1)
        for index in range(BASIS):
            vector = slab.inside(vector, first, wide)
            margin = (wide - own) // 2
            part = vector
            if margin:
                part = pltpu.roll(vector, vector.shape[1] - margin, 1)
            part = jnp.where(lane < own, part[:, 0:LANES], 0.0)
            basis[index] = part
            v_ref[:, index * own : (index + 1) * own] = part[:, 0:own]
            if index + 1 < BASIS:
                vector = slab.operate(vector, first, wide)
                first = first + 2 * half
                wide = wide - 4 * half

        lane8 = lax.broadcasted_iota(jnp.int32, (8, LANES), 1)
        sub8 = lax.broadcasted_iota(jnp.int32, (8, LANES), 0)
        gram = jnp.zeros((8, LANES), jnp.float32)
        for slot, (i, j) in enumerate(PAIRS):
            value = two_prod(basis[i], basis[j])
            count = rows
            while count > 8:
                count //= 2
                value = dd_add(
                    (value[0][:count], value[1][:count]), (value[0][count:], value[1][count:])
                )
            for axis, size in ((0, 8), (1, LANES)):
                step = size // 2
                while step:
                    value = dd_add(
                        value, tuple(pltpu.roll(part, step, axis) for part in value)
                    )
                    step //= 2
            gram = jnp.where((lane8 == slot) & (sub8 == 0), value[0], gram)
            gram = jnp.where((lane8 == slot) & (sub8 == 1), value[1], gram)
        g_ref[...] = gram

    return pl.pallas_call(
        body,
        in_specs=specs(pltpu.SMEM, pltpu.VMEM, pltpu.VMEM, pltpu.VMEM),
        out_specs=specs(pltpu.VMEM, pltpu.VMEM),
        out_shape=[
            jax.ShapeDtypeStruct((rows, per_row), jnp.float32),
            jax.ShapeDtypeStruct((8, LANES), jnp.float32),
        ],
        scratch_shapes=[pltpu.VMEM((BASIS, rows, LANES), jnp.float32)]
        + Slab.scratch(rows, lanes),
        name="krylov",
    )(start, b, applied, taps)


def combine(initial, vectors, grams, *, own):
    members = grams.shape[0]

    def body(x_ref, v_ref, g_ref, o_ref, r_ref):
        high = jnp.concatenate([g_ref[m, 0:1] for m in range(members)], axis=0)
        low = jnp.concatenate([g_ref[m, 1:2] for m in range(members)], axis=0)
        total = (high, low)
        count = members
        while count > 1:
            count //= 2
            total = dd_add(
                (total[0][:count], total[1][:count]), (total[0][count:], total[1][count:])
            )
        entries = {}
        for slot, (i, j) in enumerate(PAIRS):
            entry = tuple(
                jnp.broadcast_to(part[:, slot : slot + 1], (1, LANES)) for part in total
            )
            entries[i, j] = entries[j, i] = entry

        def inner(p, q, ahead):
            result = None
            for i, a in enumerate(p):
                row = None
                for j, b in enumerate(q):
                    term = dd_mul(b, entries[i, j + ahead])
                    row = term if row is None else dd_add(row, term)
                row = dd_mul(a, row)
                result = row if result is None else dd_add(result, row)
            return result

        one = (jnp.ones((1, LANES), jnp.float32), jnp.zeros((1, LANES), jnp.float32))
        residual = [one]
        direction = [one]
        template = []
        norm_now = entries[0, 0]
        for iteration in range(ITERS):
            step_size = dd_div(norm_now, inner(direction, direction, 1))
            moved = [dd_mul(step_size, d) for d in direction]
            template = [dd_add(t, m) for t, m in zip(template, moved)] + moved[len(template) :]
            residual = (
                residual[:1]
                + [dd_add(r, dd_neg(m)) for r, m in zip(residual[1:], moved)]
                + [dd_neg(m) for m in moved[len(residual) - 1 :]]
            )
            if iteration + 1 < ITERS:
                norm_next = inner(residual, residual, 0)
                ratio = dd_div(norm_next, norm_now)
                scaled = [dd_mul(ratio, d) for d in direction]
                direction = [dd_add(r, s) for r, s in zip(residual, scaled)] + residual[
                    len(scaled) :
                ]
                norm_now = norm_next
        for slab in range(vectors.shape[0]):
            place = slice(slab * own, (slab + 1) * own)
            parts = [v_ref[slab, :, k * own : (k + 1) * own] for k in range(BASIS)]
            final = x_ref[:, place]
            for weight, part in zip(template, parts):
                final = final + weight[0][:, 0:1] * part
            rest = residual[0][0][:, 0:1] * parts[0]
            for weight, part in zip(residual[1:], parts[1:]):
                rest = rest + weight[0][:, 0:1] * part
            o_ref[:, place] = final
            r_ref[:, place] = rest

    return pl.pallas_call(
        body,
        in_specs=specs(pltpu.VMEM, pltpu.VMEM, pltpu.VMEM),
        out_specs=specs(pltpu.VMEM, pltpu.VMEM),
        out_shape=[jax.ShapeDtypeStruct(initial.shape, jnp.float32)] * 2,
        name="combine",
    )(initial, vectors, grams)


def on_device(right_side, initial_guess, kernel):
    tile_rows, tile_cols = initial_guess.shape
    row_count = lax.axis_size("row")
    col_count = lax.axis_size("col")
    half = kernel.shape[0] // 2
    own = tile_cols // row_count
    halo = 2 * half * BASIS
    side = halo - 2 * half
    x_lanes = round_up(own + 2 * halo, LANES)
    b_lanes = round_up(own + 2 * side, LANES)

    up = [(i, i + 1) for i in range(col_count - 1)]
    down = [(j, i) for i, j in up]

    def gather(tile, margin, lanes):
        before = lax.ppermute(tile[:, -margin:], "col", up)
        after = lax.ppermute(tile[:, :margin], "col", down)
        wide = jnp.concatenate([before, tile, after], axis=1)
        missing = (row_count - 1) * own + lanes - wide.shape[1]
        wide = jnp.pad(wide, ((0, 0), (0, max(0, missing))))
        blocks = jnp.stack([wide[:, i * own : i * own + lanes] for i in range(row_count)])
        slab = lax.all_to_all(blocks, "row", 0, 0)
        return slab.reshape(row_count * tile_rows, lanes)

    tables = toeplitz_tables(kernel)
    x = gather(initial_guess, halo, x_lanes)
    b = gather(right_side, side, b_lanes)
    start = lax.axis_index("col") * tile_cols + lax.axis_index("row") * own - halo
    start = start.astype(jnp.int32).reshape(1)
    columns = col_count * tile_cols
    applied, taps = apply_first(
        x, tables, start, half=half, columns=columns, width=own + 2 * halo
    )
    vectors, gram = krylov(
        b,
        applied,
        taps,
        start + 2 * half,
        half=half,
        own=own,
        columns=columns,
        width=own + 2 * side,
    )
    back = lax.all_to_all(vectors.reshape(row_count, tile_rows, BASIS * own), "row", 0, 0)
    members = row_count * col_count
    sent = jnp.broadcast_to(gram[None], (members,) + gram.shape)
    grams = lax.all_to_all(sent, ("row", "col"), 0, 0)
    return tuple(combine(initial_guess, back, grams, own=own))


def solution(mesh):
    placed = (P("row", "col"), P("row", "col"), P())
    return jax.shard_map(
        on_device,
        mesh=mesh,
        in_specs=placed,
        out_specs=(P("row", "col"), P("row", "col")),
        check_vma=False,
    )
```

```python
import math

import jax
import jax.numpy as jnp
from jax import lax
from jax.experimental import pallas as pl
from jax.experimental.pallas import tpu as pltpu
from jax.sharding import PartitionSpec as P

ITERS = 3
PENALTY = 0.05
LANES = 128
SHIFTS = 4
BLOCK = 32
BAND = 64
UNROLL = 8
EDGE = 16
BASIS = ITERS + 1
PAIRS = [(i, j) for i in range(BASIS) for j in range(i, BASIS)]


def round_up(value, step):
    return -(-value // step) * step


def two_sum(a, b):
    s = a + b
    t = s - a
    return s, (a - (s - t)) + (b - t)


def halves(a):
    c = a * 4097.0
    high = c - (c - a)
    return high, a - high


def two_prod(a, b):
    p = a * b
    ah, al = halves(a)
    bh, bl = halves(b)
    return p, ((ah * bh - p) + ah * bl + al * bh) + al * bl


def dd_add(x, y):
    s, e = two_sum(x[0], y[0])
    return two_sum(s, e + (x[1] + y[1]))


def dd_mul(x, y):
    p, e = two_prod(x[0], y[0])
    return two_sum(p, e + (x[0] * y[1] + x[1] * y[0]))


def dd_neg(x):
    return -x[0], -x[1]


def dd_div(x, y):
    q = x[0] / y[0]
    rest = dd_add(x, dd_neg(dd_mul((q, jnp.zeros_like(q)), y)))
    return two_sum(q, rest[0] / y[0])


def toeplitz_tables(taps):
    width = taps.shape[0]
    groups = -(-width // SHIFTS)
    skip = EDGE - width // 2
    tap = jnp.arange(width, dtype=jnp.int32)[:, None, None]
    row = jnp.arange(BLOCK, dtype=jnp.int32)[None, :, None]
    band = jnp.arange(BAND, dtype=jnp.int32)[None, None, :]
    selector = (band - row - skip == tap).astype(jnp.float32)
    both = jnp.stack([taps, taps[::-1, ::-1]])
    both = jnp.pad(both, ((0, 0), (0, 0), (0, groups * SHIFTS - width)))
    both = both.reshape(2, width, groups, SHIFTS)
    tables = jnp.einsum("zags,arq->zgrsq", both, selector, precision=lax.Precision.HIGHEST)
    return tables.reshape(2, groups * BLOCK, SHIFTS * BAND)


class Slab:
    def __init__(self, rows, half, columns, pad, stack, out, smooth, taps):
        self.rows, self.half, self.columns = rows, half, columns
        self.pad, self.stack, self.out, self.smooth, self.taps = pad, stack, out, smooth, taps
        lanes = pad.shape[1]
        pad[0:EDGE, :] = jnp.zeros((EDGE, lanes), jnp.float32)
        pad[EDGE + rows :, :] = jnp.zeros((EDGE, lanes), jnp.float32)

    @staticmethod
    def scratch(rows, lanes):
        tall = rows + 2 * EDGE
        return [
            pltpu.VMEM((tall, lanes), jnp.float32),
            pltpu.VMEM((2, SHIFTS, tall, lanes), jnp.bfloat16),
            pltpu.VMEM((rows, lanes), jnp.float32),
            pltpu.VMEM((rows, lanes), jnp.float32),
        ]

    def correlate(self, which, lanes):
        pad, stack, out, taps = self.pad, self.stack, self.out, self.taps
        groups = taps.shape[1] // BLOCK
        for shift in range(SHIFTS):
            moved = pad[:, 0:lanes]
            if shift:
                moved = pltpu.roll(moved, lanes - shift, 1)
            high = moved.astype(jnp.bfloat16)
            stack[0, shift, :, 0:lanes] = high
            stack[1, shift, :, 0:lanes] = (moved - high.astype(jnp.float32)).astype(jnp.bfloat16)

        count = self.rows // BLOCK
        beside = 2 if lanes % (2 * LANES) and count % 2 == 0 else 1
        together = math.gcd(count, UNROLL)

        def some(block):
            bases = [pl.multiple_of((block + i) * BLOCK, BLOCK) for i in range(beside)]
            operand = jnp.concatenate(
                [
                    jnp.concatenate(
                        [stack[part, shift, pl.ds(base, BAND), 0:lanes] for base in bases], axis=1
                    )
                    for part in (0, 0, 1)
                    for shift in range(SHIFTS)
                ],
                axis=0,
            )
            acc = jnp.dot(taps[which], operand, preferred_element_type=jnp.float32)
            for index, base in enumerate(bases):
                columns = slice(index * lanes, (index + 1) * lanes)
                total = acc[(groups - 1) * BLOCK :, columns]
                for group in range(groups - 2, -1, -1):
                    total = acc[group * BLOCK : (group + 1) * BLOCK, columns] + pltpu.roll(
                        total, lanes - SHIFTS, 1
                    )
                out[pl.ds(base, BLOCK), 0:lanes] = total

        def step(turn, carry):
            for index in range(0, together, beside):
                some(together * turn + index)
            return carry

        lax.fori_loop(0, count // together, step, 0)

    def inside(self, value, first, width):
        lane = lax.broadcasted_iota(jnp.int32, value.shape, 1)
        position = lane + first
        keep = (position >= 0) & (position < self.columns) & (lane < width)
        return jnp.where(keep, value, 0.0)

    def operate(self, source, first, width):
        rows, half, pad = self.rows, self.half, self.pad
        lanes = round_up(width, LANES)
        pad[EDGE : EDGE + rows, 0:lanes] = source
        center = pad[EDGE : EDGE + rows, 0:lanes]
        lap = (
            4.0 * center
            - pad[EDGE - 1 : EDGE - 1 + rows, 0:lanes]
            - pad[EDGE + 1 : EDGE + 1 + rows, 0:lanes]
            - pltpu.roll(center, 1, 1)
            - pltpu.roll(center, lanes - 1, 1)
        )
        self.smooth[:, 0:lanes] = PENALTY * pltpu.roll(lap, lanes - 2 * half, 1)
        self.correlate(0, lanes)
        inner = width - 2 * half
        lanes_in = round_up(inner, LANES)
        pad[EDGE : EDGE + rows, 0:lanes_in] = self.inside(
            self.out[:, 0:lanes_in], first + half, inner
        )
        self.correlate(1, lanes_in)
        last = width - 4 * half
        lanes_out = round_up(last, LANES)
        return self.out[:, 0:lanes_out] + self.smooth[:, 0:lanes_out]


def specs(*spaces):
    return [pl.BlockSpec(memory_space=space) for space in spaces]


def apply_first(x, tables, start, *, half, columns, width):
    rows, lanes = x.shape
    span = tables.shape[2]
    last = round_up(width - 4 * half, LANES)

    def body(start_ref, x_ref, t_ref, o_ref, taps, *scratch):
        for which in range(2):
            full = t_ref[which]
            high = full.astype(jnp.bfloat16)
            low = (full - high.astype(jnp.float32)).astype(jnp.bfloat16)
            taps[which, :, 0:span] = high
            taps[which, :, span : 2 * span] = low
            taps[which, :, 2 * span : 3 * span] = high
        slab = Slab(rows, half, columns, *scratch, taps)
        o_ref[...] = slab.operate(x_ref[...], start_ref[0], width)

    return pl.pallas_call(
        body,
        in_specs=specs(pltpu.SMEM, pltpu.VMEM, pltpu.VMEM),
        out_specs=specs(pltpu.VMEM, pltpu.VMEM),
        out_shape=[
            jax.ShapeDtypeStruct((rows, last), jnp.float32),
            jax.ShapeDtypeStruct((2, tables.shape[1], 3 * span), jnp.bfloat16),
        ],
        scratch_shapes=Slab.scratch(rows, lanes),
        name="apply_first",
    )(start, x, tables)


def krylov(b, applied, taps, start, *, half, own, columns, width, parts):
    rows, lanes = b.shape
    part_rows = rows // parts
    per_row = round_up(BASIS * own, LANES)

    def body(start_ref, b_ref, a_ref, t_ref, v_ref, basis, *scratch):
        slab = Slab(rows, half, columns, *scratch, t_ref)
        first = start_ref[0]
        wide = width
        vector = b_ref[...] - a_ref[...]
        lane = lax.broadcasted_iota(jnp.int32, (rows, LANES), 1)
        for index in range(BASIS):
            vector = slab.inside(vector, first, wide)
            margin = (wide - own) // 2
            part = vector
            if margin:
                part = pltpu.roll(vector, vector.shape[1] - margin, 1)
            part = jnp.where(lane < own, part[:, 0:LANES], 0.0)
            basis[index] = part
            for cut in range(parts):
                v_ref[cut, 0:part_rows, index * own : (index + 1) * own] = part[
                    cut * part_rows : (cut + 1) * part_rows, 0:own
                ]
            if index + 1 < BASIS:
                vector = slab.operate(vector, first, wide)
                first = first + 2 * half
                wide = wide - 4 * half

        lane8 = lax.broadcasted_iota(jnp.int32, (8, LANES), 1)
        sub8 = lax.broadcasted_iota(jnp.int32, (8, LANES), 0)
        gram = jnp.zeros((8, LANES), jnp.float32)
        for slot, (i, j) in enumerate(PAIRS):
            value = two_prod(basis[i], basis[j])
            count = rows
            while count > 8:
                count //= 2
                value = dd_add(
                    (value[0][:count], value[1][:count]), (value[0][count:], value[1][count:])
                )
            for axis, size in ((0, 8), (1, LANES)):
                step = size // 2
                while step:
                    value = dd_add(
                        value, tuple(pltpu.roll(part, step, axis) for part in value)
                    )
                    step //= 2
            gram = jnp.where((lane8 == slot) & (sub8 == 0), value[0], gram)
            gram = jnp.where((lane8 == slot) & (sub8 == 1), value[1], gram)
        for cut in range(parts):
            v_ref[cut, part_rows:, :] = jnp.zeros((8, per_row), jnp.float32)
            v_ref[cut, part_rows:, 0:LANES] = gram

    return pl.pallas_call(
        body,
        in_specs=specs(pltpu.SMEM, pltpu.VMEM, pltpu.VMEM, pltpu.VMEM),
        out_specs=pl.BlockSpec(memory_space=pltpu.VMEM),
        out_shape=jax.ShapeDtypeStruct((parts, part_rows + 8, per_row), jnp.float32),
        scratch_shapes=[pltpu.VMEM((BASIS, rows, LANES), jnp.float32)]
        + Slab.scratch(rows, lanes),
        name="krylov",
    )(start, b, applied, taps)


def combine(initial, vectors, grams, *, own):
    members = grams.shape[0]
    tile_rows = initial.shape[0]

    def body(x_ref, v_ref, g_ref, o_ref, r_ref):
        count = grams.shape[1] // 2
        total = (g_ref[0, 0:count], g_ref[0, count:])
        for member in range(1, members):
            total = dd_add(total, (g_ref[member, 0:count], g_ref[member, count:]))
        while count > 1:
            count //= 2
            total = dd_add(
                (total[0][:count], total[1][:count]), (total[0][count:], total[1][count:])
            )
        entries = {}
        for slot, (i, j) in enumerate(PAIRS):
            entry = tuple(
                jnp.broadcast_to(part[:, slot : slot + 1], (1, LANES)) for part in total
            )
            entries[i, j] = entries[j, i] = entry

        def inner(p, q, ahead):
            result = None
            for i, a in enumerate(p):
                row = None
                for j, b in enumerate(q):
                    term = dd_mul(b, entries[i, j + ahead])
                    row = term if row is None else dd_add(row, term)
                row = dd_mul(a, row)
                result = row if result is None else dd_add(result, row)
            return result

        one = (jnp.ones((1, LANES), jnp.float32), jnp.zeros((1, LANES), jnp.float32))
        residual = [one]
        direction = [one]
        template = []
        norm_now = entries[0, 0]
        for iteration in range(ITERS):
            step_size = dd_div(norm_now, inner(direction, direction, 1))
            moved = [dd_mul(step_size, d) for d in direction]
            template = [dd_add(t, m) for t, m in zip(template, moved)] + moved[len(template) :]
            residual = (
                residual[:1]
                + [dd_add(r, dd_neg(m)) for r, m in zip(residual[1:], moved)]
                + [dd_neg(m) for m in moved[len(residual) - 1 :]]
            )
            if iteration + 1 < ITERS:
                norm_next = inner(residual, residual, 0)
                ratio = dd_div(norm_next, norm_now)
                scaled = [dd_mul(ratio, d) for d in direction]
                direction = [dd_add(r, s) for r, s in zip(residual, scaled)] + residual[
                    len(scaled) :
                ]
                norm_now = norm_next
        for slab in range(vectors.shape[0]):
            place = slice(slab * own, (slab + 1) * own)
            parts = [v_ref[slab, 0:tile_rows, k * own : (k + 1) * own] for k in range(BASIS)]
            final = x_ref[:, place]
            for weight, part in zip(template, parts):
                final = final + weight[0][:, 0:1] * part
            rest = residual[0][0][:, 0:1] * parts[0]
            for weight, part in zip(residual[1:], parts[1:]):
                rest = rest + weight[0][:, 0:1] * part
            o_ref[:, place] = final
            r_ref[:, place] = rest

    return pl.pallas_call(
        body,
        in_specs=specs(pltpu.VMEM, pltpu.VMEM, pltpu.VMEM),
        out_specs=specs(pltpu.VMEM, pltpu.VMEM),
        out_shape=[jax.ShapeDtypeStruct(initial.shape, jnp.float32)] * 2,
        name="combine",
    )(initial, vectors, grams)


def on_device(right_side, initial_guess, kernel):
    tile_rows, tile_cols = initial_guess.shape
    row_count = lax.axis_size("row")
    col_count = lax.axis_size("col")
    half = kernel.shape[0] // 2
    own = tile_cols // row_count
    halo = 2 * half * BASIS
    side = halo - 2 * half
    x_lanes = round_up(own + 2 * halo, LANES)
    b_lanes = round_up(own + 2 * side, LANES)

    up = [(i, i + 1) for i in range(col_count - 1)]
    down = [(j, i) for i, j in up]

    tables = toeplitz_tables(kernel)
    right_edge = jnp.concatenate([initial_guess[:, -halo:], right_side[:, -side:]], axis=1)
    left_edge = jnp.concatenate([initial_guess[:, :halo], right_side[:, :side]], axis=1)
    before = lax.ppermute(right_edge, "col", up)
    after = lax.ppermute(left_edge, "col", down)

    def gather(left, tile, right, lanes):
        wide = jnp.concatenate([left, tile, right], axis=1)
        missing = (row_count - 1) * own + lanes - wide.shape[1]
        wide = jnp.pad(wide, ((0, 0), (0, max(0, missing))))
        blocks = jnp.stack([wide[:, i * own : i * own + lanes] for i in range(row_count)])
        slab = lax.all_to_all(blocks, "row", 0, 0)
        return slab.reshape(row_count * tile_rows, lanes)

    x = gather(before[:, :halo], initial_guess, after[:, :halo], x_lanes)
    right_side, tables = lax.optimization_barrier((right_side, tables))
    b = gather(before[:, halo:], right_side, after[:, halo:], b_lanes)
    start = lax.axis_index("col") * tile_cols + lax.axis_index("row") * own - halo
    start = start.astype(jnp.int32).reshape(1)
    columns = col_count * tile_cols
    applied, taps = apply_first(
        x, tables, start, half=half, columns=columns, width=own + 2 * halo
    )
    vectors = krylov(
        b,
        applied,
        taps,
        start + 2 * half,
        half=half,
        own=own,
        columns=columns,
        width=own + 2 * side,
        parts=row_count,
    )
    back = lax.all_to_all(vectors, "row", 0, 0)
    gram = jnp.concatenate(
        [back[:, tile_rows + part, 0:LANES] for part in range(2)], axis=0
    )
    sent = jnp.broadcast_to(gram[None], (col_count,) + gram.shape)
    grams = lax.all_to_all(sent, "col", 0, 0)
    return tuple(combine(initial_guess, back, grams, own=own))


def solution(mesh):
    placed = (P("row", "col"), P("row", "col"), P())
    return jax.shard_map(
        on_device,
        mesh=mesh,
        in_specs=placed,
        out_specs=(P("row", "col"), P("row", "col")),
        check_vma=False,
    )
```

```python
import math

import jax
import jax.numpy as jnp
from jax import lax
from jax.experimental import pallas as pl
from jax.experimental.pallas import tpu as pltpu
from jax.sharding import PartitionSpec as P

ITERS = 3
PENALTY = 0.05
LANES = 128
SHIFTS = 4
BLOCK = 32
BAND = 64
UNROLL = 8
EDGE = 16
BASIS = ITERS + 1
PAIRS = [(i, j) for i in range(BASIS) for j in range(i, BASIS)]


def round_up(value, step):
    return -(-value // step) * step


def two_sum(a, b):
    s = a + b
    t = s - a
    return s, (a - (s - t)) + (b - t)


def halves(a):
    c = a * 4097.0
    high = c - (c - a)
    return high, a - high


def two_prod(a, b):
    p = a * b
    ah, al = halves(a)
    bh, bl = halves(b)
    return p, ((ah * bh - p) + ah * bl + al * bh) + al * bl


def dd_add(x, y):
    s, e = two_sum(x[0], y[0])
    return two_sum(s, e + (x[1] + y[1]))


def dd_mul(x, y):
    p, e = two_prod(x[0], y[0])
    return two_sum(p, e + (x[0] * y[1] + x[1] * y[0]))


def dd_neg(x):
    return -x[0], -x[1]


def dd_div(x, y):
    q = x[0] / y[0]
    rest = dd_add(x, dd_neg(dd_mul((q, jnp.zeros_like(q)), y)))
    return two_sum(q, rest[0] / y[0])


def toeplitz_tables(taps):
    width = taps.shape[0]
    groups = -(-width // SHIFTS)
    skip = EDGE - width // 2
    tap = jnp.arange(width, dtype=jnp.int32)[:, None, None]
    row = jnp.arange(BLOCK, dtype=jnp.int32)[None, :, None]
    band = jnp.arange(BAND, dtype=jnp.int32)[None, None, :]
    selector = (band - row - skip == tap).astype(jnp.float32)
    both = jnp.stack([taps, taps[::-1, ::-1]])
    both = jnp.pad(both, ((0, 0), (0, 0), (0, groups * SHIFTS - width)))
    both = both.reshape(2, width, groups, SHIFTS)
    tables = jnp.einsum("zags,arq->zgrsq", both, selector, precision=lax.Precision.HIGHEST)
    return tables.reshape(2, groups * BLOCK, SHIFTS * BAND)


class Slab:
    def __init__(self, rows, half, columns, pad, stack, out, smooth, taps):
        self.rows, self.half, self.columns = rows, half, columns
        self.pad, self.stack, self.out, self.smooth, self.taps = pad, stack, out, smooth, taps
        lanes = pad.shape[1]
        pad[0:EDGE, :] = jnp.zeros((EDGE, lanes), jnp.float32)
        pad[EDGE + rows :, :] = jnp.zeros((EDGE, lanes), jnp.float32)

    @staticmethod
    def scratch(rows, lanes):
        tall = rows + 2 * EDGE
        return [
            pltpu.VMEM((tall, lanes), jnp.float32),
            pltpu.VMEM((2, SHIFTS, tall, lanes), jnp.bfloat16),
            pltpu.VMEM((rows, lanes), jnp.float32),
            pltpu.VMEM((rows, lanes), jnp.float32),
        ]

    def correlate(self, which, lanes):
        pad, stack, out, taps = self.pad, self.stack, self.out, self.taps
        groups = taps.shape[1] // BLOCK
        for shift in range(SHIFTS):
            moved = pad[:, 0:lanes]
            if shift:
                moved = pltpu.roll(moved, lanes - shift, 1)
            high = moved.astype(jnp.bfloat16)
            stack[0, shift, :, 0:lanes] = high
            stack[1, shift, :, 0:lanes] = (moved - high.astype(jnp.float32)).astype(jnp.bfloat16)

        count = self.rows // BLOCK
        beside = 2 if lanes % (2 * LANES) and count % 2 == 0 else 1
        together = math.gcd(count, UNROLL)

        def some(block):
            bases = [(block + i) * BLOCK for i in range(beside)]
            if not isinstance(block, int):
                bases = [pl.multiple_of(base, BLOCK) for base in bases]
            operand = jnp.concatenate(
                [
                    jnp.concatenate(
                        [stack[part, shift, pl.ds(base, BAND), 0:lanes] for base in bases], axis=1
                    )
                    for part in (0, 0, 1)
                    for shift in range(SHIFTS)
                ],
                axis=0,
            )
            acc = jnp.dot(taps[which], operand, preferred_element_type=jnp.float32)
            for index, base in enumerate(bases):
                columns = slice(index * lanes, (index + 1) * lanes)
                total = acc[(groups - 1) * BLOCK :, columns]
                for group in range(groups - 2, -1, -1):
                    total = acc[group * BLOCK : (group + 1) * BLOCK, columns] + pltpu.roll(
                        total, lanes - SHIFTS, 1
                    )
                out[pl.ds(base, BLOCK), 0:lanes] = total

        def step(turn, carry):
            for index in range(0, together, beside):
                some(together * turn + index)
            return carry

        if count == together:
            step(0, 0)
        else:
            lax.fori_loop(0, count // together, step, 0)

    def inside(self, value, first, width):
        lane = lax.broadcasted_iota(jnp.int32, value.shape, 1)
        position = lane + first
        keep = (position >= 0) & (position < self.columns) & (lane < width)
        return jnp.where(keep, value, 0.0)

    def operate(self, source, first, width):
        rows, half, pad = self.rows, self.half, self.pad
        lanes = round_up(width, LANES)
        pad[EDGE : EDGE + rows, 0:lanes] = source
        center = pad[EDGE : EDGE + rows, 0:lanes]
        lap = (
            4.0 * center
            - pad[EDGE - 1 : EDGE - 1 + rows, 0:lanes]
            - pad[EDGE + 1 : EDGE + 1 + rows, 0:lanes]
            - pltpu.roll(center, 1, 1)
            - pltpu.roll(center, lanes - 1, 1)
        )
        self.smooth[:, 0:lanes] = PENALTY * pltpu.roll(lap, lanes - 2 * half, 1)
        self.correlate(0, lanes)
        inner = width - 2 * half
        lanes_in = round_up(inner, LANES)
        pad[EDGE : EDGE + rows, 0:lanes_in] = self.inside(
            self.out[:, 0:lanes_in], first + half, inner
        )
        self.correlate(1, lanes_in)
        last = width - 4 * half
        lanes_out = round_up(last, LANES)
        return self.out[:, 0:lanes_out] + self.smooth[:, 0:lanes_out]


def specs(*spaces):
    return [pl.BlockSpec(memory_space=space) for space in spaces]


def apply_first(x, tables, start, *, half, columns, width):
    rows, lanes = x.shape
    span = tables.shape[2]
    last = round_up(width - 4 * half, LANES)

    def body(start_ref, x_ref, t_ref, o_ref, taps, *scratch):
        for which in range(2):
            full = t_ref[which]
            high = full.astype(jnp.bfloat16)
            low = (full - high.astype(jnp.float32)).astype(jnp.bfloat16)
            taps[which, :, 0:span] = high
            taps[which, :, span : 2 * span] = low
            taps[which, :, 2 * span : 3 * span] = high
        slab = Slab(rows, half, columns, *scratch, taps)
        o_ref[...] = slab.operate(x_ref[...], start_ref[0], width)

    return pl.pallas_call(
        body,
        in_specs=specs(pltpu.SMEM, pltpu.VMEM, pltpu.VMEM),
        out_specs=specs(pltpu.VMEM, pltpu.VMEM),
        out_shape=[
            jax.ShapeDtypeStruct((rows, last), jnp.float32),
            jax.ShapeDtypeStruct((2, tables.shape[1], 3 * span), jnp.bfloat16),
        ],
        scratch_shapes=Slab.scratch(rows, lanes),
        name="apply_first",
    )(start, x, tables)


def krylov(b, applied, taps, start, *, half, own, columns, width, parts):
    rows, lanes = b.shape
    part_rows = rows // parts
    per_row = round_up(BASIS * own, LANES)

    def body(start_ref, b_ref, a_ref, t_ref, v_ref, basis, *scratch):
        slab = Slab(rows, half, columns, *scratch, t_ref)
        first = start_ref[0]
        wide = width
        vector = b_ref[...] - a_ref[...]
        lane = lax.broadcasted_iota(jnp.int32, (rows, LANES), 1)
        for index in range(BASIS):
            vector = slab.inside(vector, first, wide)
            margin = (wide - own) // 2
            part = vector
            if margin:
                part = pltpu.roll(vector, vector.shape[1] - margin, 1)
            part = jnp.where(lane < own, part[:, 0:LANES], 0.0)
            basis[index] = part
            for cut in range(parts):
                v_ref[cut, 0:part_rows, index * own : (index + 1) * own] = part[
                    cut * part_rows : (cut + 1) * part_rows, 0:own
                ]
            if index + 1 < BASIS:
                vector = slab.operate(vector, first, wide)
                first = first + 2 * half
                wide = wide - 4 * half

        lane8 = lax.broadcasted_iota(jnp.int32, (8, LANES), 1)
        sub8 = lax.broadcasted_iota(jnp.int32, (8, LANES), 0)
        gram = jnp.zeros((8, LANES), jnp.float32)
        for slot, (i, j) in enumerate(PAIRS):
            value = two_prod(basis[i], basis[j])
            count = rows
            while count > 8:
                count //= 2
                value = dd_add(
                    (value[0][:count], value[1][:count]), (value[0][count:], value[1][count:])
                )
            for axis, size in ((0, 8), (1, LANES)):
                step = size // 2
                while step:
                    value = dd_add(
                        value, tuple(pltpu.roll(part, step, axis) for part in value)
                    )
                    step //= 2
            gram = jnp.where((lane8 == slot) & (sub8 == 0), value[0], gram)
            gram = jnp.where((lane8 == slot) & (sub8 == 1), value[1], gram)
        for cut in range(parts):
            v_ref[cut, part_rows:, :] = jnp.zeros((8, per_row), jnp.float32)
            v_ref[cut, part_rows:, 0:LANES] = gram

    return pl.pallas_call(
        body,
        in_specs=specs(pltpu.SMEM, pltpu.VMEM, pltpu.VMEM, pltpu.VMEM),
        out_specs=pl.BlockSpec(memory_space=pltpu.VMEM),
        out_shape=jax.ShapeDtypeStruct((parts, part_rows + 8, per_row), jnp.float32),
        scratch_shapes=[pltpu.VMEM((BASIS, rows, LANES), jnp.float32)]
        + Slab.scratch(rows, lanes),
        name="krylov",
    )(start, b, applied, taps)


def combine(initial, vectors, grams, *, own):
    members = grams.shape[0]
    tile_rows = initial.shape[0]

    def body(x_ref, v_ref, g_ref, o_ref, r_ref):
        count = grams.shape[1] // 2
        total = (g_ref[0, 0:count], g_ref[0, count:])
        for member in range(1, members):
            total = dd_add(total, (g_ref[member, 0:count], g_ref[member, count:]))
        while count > 1:
            count //= 2
            total = dd_add(
                (total[0][:count], total[1][:count]), (total[0][count:], total[1][count:])
            )
        entries = {}
        for slot, (i, j) in enumerate(PAIRS):
            entry = tuple(
                jnp.broadcast_to(part[:, slot : slot + 1], (1, LANES)) for part in total
            )
            entries[i, j] = entries[j, i] = entry

        def inner(p, q, ahead):
            result = None
            for i, a in enumerate(p):
                row = None
                for j, b in enumerate(q):
                    term = dd_mul(b, entries[i, j + ahead])
                    row = term if row is None else dd_add(row, term)
                row = dd_mul(a, row)
                result = row if result is None else dd_add(result, row)
            return result

        one = (jnp.ones((1, LANES), jnp.float32), jnp.zeros((1, LANES), jnp.float32))
        residual = [one]
        direction = [one]
        template = []
        norm_now = entries[0, 0]
        for iteration in range(ITERS):
            step_size = dd_div(norm_now, inner(direction, direction, 1))
            moved = [dd_mul(step_size, d) for d in direction]
            template = [dd_add(t, m) for t, m in zip(template, moved)] + moved[len(template) :]
            residual = (
                residual[:1]
                + [dd_add(r, dd_neg(m)) for r, m in zip(residual[1:], moved)]
                + [dd_neg(m) for m in moved[len(residual) - 1 :]]
            )
            if iteration + 1 < ITERS:
                norm_next = inner(residual, residual, 0)
                ratio = dd_div(norm_next, norm_now)
                scaled = [dd_mul(ratio, d) for d in direction]
                direction = [dd_add(r, s) for r, s in zip(residual, scaled)] + residual[
                    len(scaled) :
                ]
                norm_now = norm_next
        for slab in range(vectors.shape[0]):
            place = slice(slab * own, (slab + 1) * own)
            parts = [v_ref[slab, 0:tile_rows, k * own : (k + 1) * own] for k in range(BASIS)]
            final = x_ref[:, place]
            for weight, part in zip(template, parts):
                final = final + weight[0][:, 0:1] * part
            rest = residual[0][0][:, 0:1] * parts[0]
            for weight, part in zip(residual[1:], parts[1:]):
                rest = rest + weight[0][:, 0:1] * part
            o_ref[:, place] = final
            r_ref[:, place] = rest

    return pl.pallas_call(
        body,
        in_specs=specs(pltpu.VMEM, pltpu.VMEM, pltpu.VMEM),
        out_specs=specs(pltpu.VMEM, pltpu.VMEM),
        out_shape=[jax.ShapeDtypeStruct(initial.shape, jnp.float32)] * 2,
        name="combine",
    )(initial, vectors, grams)


def on_device(right_side, initial_guess, kernel):
    tile_rows, tile_cols = initial_guess.shape
    row_count = lax.axis_size("row")
    col_count = lax.axis_size("col")
    half = kernel.shape[0] // 2
    own = tile_cols // row_count
    halo = 2 * half * BASIS
    side = halo - 2 * half
    x_lanes = round_up(own + 2 * halo, LANES)
    b_lanes = round_up(own + 2 * side, LANES)

    up = [(i, i + 1) for i in range(col_count - 1)]
    down = [(j, i) for i, j in up]

    tables = toeplitz_tables(kernel)
    right_edge = jnp.concatenate([initial_guess[:, -halo:], right_side[:, -side:]], axis=1)
    left_edge = jnp.concatenate([initial_guess[:, :halo], right_side[:, :side]], axis=1)
    before = lax.ppermute(right_edge, "col", up)
    after = lax.ppermute(left_edge, "col", down)

    def gather(left, tile, right, lanes):
        wide = jnp.concatenate([left, tile, right], axis=1)
        missing = (row_count - 1) * own + lanes - wide.shape[1]
        wide = jnp.pad(wide, ((0, 0), (0, max(0, missing))))
        blocks = jnp.stack([wide[:, i * own : i * own + lanes] for i in range(row_count)])
        slab = lax.all_to_all(blocks, "row", 0, 0)
        return slab.reshape(row_count * tile_rows, lanes)

    x = gather(before[:, :halo], initial_guess, after[:, :halo], x_lanes)
    right_side, tables = lax.optimization_barrier((right_side, tables))
    b = gather(before[:, halo:], right_side, after[:, halo:], b_lanes)
    start = lax.axis_index("col") * tile_cols + lax.axis_index("row") * own - halo
    start = start.astype(jnp.int32).reshape(1)
    columns = col_count * tile_cols
    applied, taps = apply_first(
        x, tables, start, half=half, columns=columns, width=own + 2 * halo
    )
    vectors = krylov(
        b,
        applied,
        taps,
        start + 2 * half,
        half=half,
        own=own,
        columns=columns,
        width=own + 2 * side,
        parts=row_count,
    )
    back = lax.all_to_all(vectors, "row", 0, 0)
    gram = jnp.concatenate(
        [back[:, tile_rows + part, 0:LANES] for part in range(2)], axis=0
    )
    sent = jnp.broadcast_to(gram[None], (col_count,) + gram.shape)
    grams = lax.all_to_all(sent, "col", 0, 0)
    return tuple(combine(initial_guess, back, grams, own=own))


def solution(mesh):
    placed = (P("row", "col"), P("row", "col"), P())
    return jax.shard_map(
        on_device,
        mesh=mesh,
        in_specs=placed,
        out_specs=(P("row", "col"), P("row", "col")),
        check_vma=False,
    )
```
